128 devices in a mesh: gx: 4 (over y), gy: 4 (over x_lo, core), gz: 8 (over x_hi, z).
Axes of the slice: x: 4 (x_hi: 2, x_lo: 2; x = x_hi * 2 + x_lo), y: 4, z: 4, core: 2. Of those that a mesh axis runs over, the one named last changes fastest.
Arguments:
- phase: int32 [4, 8, 256], P('gx', 'gy', 'gz'), may hold values from 0 to 1
- lame: float32 [2, 2], replicated, may hold values from 0.3 to 10
- start: float32 [3, 32, 16, 32, 1024], P(None, None, 'gx', 'gy', 'gz'), may hold values from -6 to 6
Outputs:
- basis: float32 [3, 32, 16, 32, 1024], P(None, None, 'gx', 'gy', 'gz')
- coarse: float32 [32, 32], replicated
The draws below stay inside these ranges and needn't reach their ends.
All inputs are finite; a program needn't handle non-finite values.
Results may differ from the reference program's by a relative error of at most 0.0001.
Values sent between devices are 32-bit elements; how exact they have to be, the bound alone decides.
No kernel may reach another device: no remote copies, remote signals or barrier semaphores. Data moves between devices by JAX's collectives and lax.ppermute only.
A program may use at most 64 MiB of HBM per device.

```python
import math
import jax
import jax.numpy as jnp
from jax import lax

VECS = 32
ITERS = 3
PHASES = 2
BRICK = 4
NX = 16
NY = 32
NZ = 1024


def touch_ends(array, rng, low, high):
    place = [jax.random.randint(jax.random.fold_in(rng, axis), (), 0, length) for axis, length in enumerate(array.shape)]
    widest = array.shape.index(max(array.shape))
    next_to = place[:widest] + [(place[widest] + 1) % array.shape[widest]] + place[widest + 1:]
    return array.at[tuple(place)].set(low).at[tuple(next_to)].set(high)


def steps_of(own_key, dims, pieces, low, top_value):
    def one(axis_at, blocks):
        draws = jax.random.uniform(jax.random.fold_in(jax.random.fold_in(own_key, 6), axis_at), (blocks,), jnp.float32, low / len(pieces), top_value / len(pieces))
        return jnp.repeat(jnp.exp(draws), dims[axis_at] // blocks).reshape((-1,) + (1,) * (len(dims) - axis_at - 1))

    gain = one(*pieces[0])
    for cut in pieces[1:]:
        gain = gain * one(*cut)
    return gain


def normal_values(key, shape, spread, reach, split=(), kind=jnp.bfloat16):
    values = jax.random.normal(key, shape, jnp.float32) * spread
    if len(split) > 0:
        values = steps_of(key, shape, split, -0.22, 0.18) * values
    return jnp.clip(values, min=-reach, max=reach).astype(kind)


def setup_inputs(seed: int = 0) -> dict:
    key_list = jax.random.split(jax.random.key(seed), 4)
    phase = touch_ends(jax.random.randint(key_list[0], (NX // BRICK, NY // BRICK, NZ // BRICK), 0, PHASES), jax.random.fold_in(key_list[0], 1), 0, PHASES - 1).astype(jnp.int32)
    lame = jnp.clip(jnp.exp(jax.random.uniform(key_list[1], (PHASES, 2), jnp.float32, math.log(0.3), math.log(10.0))), 0.3, 10.0)
    start = normal_values(key_list[2], (3, VECS, NX, NY, NZ), 1.0, 6.0, ((2, 4), (3, 4), (4, 8)), jnp.float32)
    return dict(phase=phase, lame=lame, start=start)


def node_fields(padded_bricks, lame):
    nodes = jnp.repeat(jnp.repeat(jnp.repeat(padded_bricks, BRICK, 0), BRICK, 1), BRICK, 2)
    cut = BRICK - 1
    nodes = nodes[cut:-cut, cut:-cut, cut:-cut]
    shear = jnp.zeros(nodes.shape, jnp.float32)
    first = jnp.zeros(nodes.shape, jnp.float32)
    for index in range(PHASES):
        hit = nodes == index
        shear = shear + jnp.where(hit, lame[index, 0], 0.0)
        first = first + jnp.where(hit, lame[index, 1], 0.0)
    return (shear, first + shear)

def stencil(padded, shear, grow):
    centre = padded[:, :, 1:-1, 1:-1, 1:-1]
    shear_c = shear[1:-1, 1:-1, 1:-1]
    grow_c = grow[1:-1, 1:-1, 1:-1]
    total = jnp.zeros(centre.shape, centre.dtype)
    for axis_d in range(3):
        length = centre.shape[2 + axis_d]
        for offset in (0, 2):
            cuts = [slice(1, -1), slice(1, -1), slice(1, -1)]
            cuts[axis_d] = slice(offset, offset + length)
            cuts = tuple(cuts)
            beside = padded[(slice(None), slice(None)) + cuts]
            w_shear = 0.5 * (shear_c + shear[cuts])
            w_grow = 0.5 * (grow_c + grow[cuts])
            weight = jnp.stack([w_shear + w_grow if comp == axis_d else w_shear for comp in range(3)])
            total = total + weight[:, None] * (centre - beside)
    return total

def inner(left, right):
    return jnp.einsum('ckxyz,clxyz->kl', left, right, precision=lax.Precision.HIGHEST)

def inverse_factor(gram):
    lower_f = jnp.linalg.cholesky(gram)
    return lax.linalg.triangular_solve(lower_f, jnp.eye(gram.shape[0], dtype=jnp.float32), left_side=True, lower=True)

def reference(phase, lame, start):
    total_rows = 3.0 * start.shape[2] * start.shape[3] * start.shape[4]
    shear, grow = node_fields(jnp.pad(phase, 1), lame)
    widths = ((0, 0), (0, 0), (1, 1), (1, 1), (1, 1))
    block = start
    for step in range(ITERS):
        image = stencil(jnp.pad(block, widths), shear, grow)
        factor = inverse_factor(inner(image, image) / total_rows)
        block = jnp.einsum('kl,clxyz->ckxyz', factor, image, precision=lax.Precision.HIGHEST)
    applied = stencil(jnp.pad(block, widths), shear, grow)
    return (block, inner(block, applied) / total_rows)
```

```python
import jax
import jax.numpy as jnp
from jax import lax
from jax.experimental import pallas as pl
from jax.experimental.pallas import tpu as pltpu
from jax.sharding import PartitionSpec as P

ITERS = 3
BRICK = 4

COMPS, VECS, NX, NY, NZ = 3, 32, 4, 8, 128
FIELD = (COMPS, VECS, NX * NY * NZ)
F32 = jnp.float32

XI, XLD, XLO, XHD, XHO = 0, 2, 4, 6, 8
YM, YLD, YLO, YHD, YHO = 10, 11, 12, 13, 14
ZLD, ZLO, ZRD, ZRO = 15, 17, 19, 21
KIND = 23
YCASE = (0, 1, 1, 2, 3, 4, 4, 5)
XCASE = (0, 1, 1, 2)

VMEM = pl.BlockSpec(memory_space=pltpu.VMEM)
SMEM = pl.BlockSpec(memory_space=pltpu.SMEM)


def in_vmem(*arrays):
    return [pltpu.with_memory_space_constraint(a, pltpu.VMEM) for a in arrays]


def lanes():
    return lax.broadcasted_iota(jnp.int32, (VECS, NZ), 1)


def rows(block):
    return pl.ds(pl.multiple_of(block * VECS, VECS), VECS)


def dot_t(a, b):
    return lax.dot_general(
        a, b, (((1,), (1,)), ((), ())), precision=lax.Precision.HIGHEST, preferred_element_type=F32
    )


def dot(a, b):
    return jnp.dot(a, b, precision=lax.Precision.HIGHEST, preferred_element_type=F32)


def emit_faces(c, xi, yi, value, faces, z_lo, z_hi, lane):
    x_lo, x_hi, y_lo, y_hi = faces
    if xi == 0:
        x_lo[rows(c * NY + yi), :] = value
    if xi == NX - 1:
        x_hi[rows(c * NY + yi), :] = value
    if yi == 0:
        y_lo[rows(c * NX + xi), :] = value
    if yi == NY - 1:
        y_hi[rows(c * NX + xi), :] = value
    block = xi * NY + yi
    low = pltpu.roll(value, block, 1) if block else value
    high = pltpu.roll(value, block + 1, 1)
    return jnp.where(lane == block, low, z_lo), jnp.where(lane == block, high, z_hi)


def pack_kernel(u_ref, phase_ref, xl, xh, yl, yh, zl, zh):
    lane = lanes()

    def comp(c, carry):
        z_lo = jnp.zeros((VECS, NZ), F32)
        z_hi = jnp.zeros((VECS, NZ), F32)
        for xi in range(NX):
            for yi in range(NY):
                at = (xi * NY + yi) * NZ
                value = u_ref[c, :, at : at + NZ]
                z_lo, z_hi = emit_faces(c, xi, yi, value, (xl, xh, yl, yh), z_lo, z_hi, lane)
        zl[rows(c), :] = z_lo
        zh[rows(c), :] = z_hi
        return carry

    lax.fori_loop(0, COMPS, comp, 0)
    spread = (
        lax.broadcasted_iota(jnp.int32, (NZ // BRICK, NZ), 1) // BRICK
        == lax.broadcasted_iota(jnp.int32, (NZ // BRICK, NZ), 0)
    ).astype(F32)
    bricks = jnp.concatenate([phase_ref[0].astype(F32), jnp.zeros((6, NZ // BRICK), F32)], axis=0)
    nodes = jnp.dot(bricks, spread, preferred_element_type=F32)
    for face, blocks in ((xl, COMPS * NY), (xh, COMPS * NY), (yl, COMPS * NX), (yh, COMPS * NX), (zl, COMPS), (zh, COMPS)):
        face[blocks * VECS : blocks * VECS + 8, :] = nodes


def weight_tables(lame_ref, own_ref, halos, w_ref, d_ref):
    hxm, hxp, hym, hyp, hzm, hzp = halos
    lane = lax.broadcasted_iota(jnp.int32, (1, NZ), 1)
    first = [lax.axis_index(a) == 0 for a in ("gx", "gy", "gz")]
    last = [lax.axis_index(a) == lax.axis_size(a) - 1 for a in ("gx", "gy", "gz")]

    def phases(ref, blocks, outside):
        found = ref[blocks * VECS : blocks * VECS + 8, :]
        found = jnp.where(outside, 0.0, found)
        return [found[j : j + 1] for j in range(2)]

    own = own_ref[...]
    own = [own[j : j + 1] for j in range(2)]
    x_m = phases(hxm, COMPS * NY, first[0])
    x_p = phases(hxp, COMPS * NY, last[0])
    y_m = phases(hym, COMPS * NX, first[1])
    y_p = phases(hyp, COMPS * NX, last[1])
    z_m = phases(hzm, COMPS, first[2])
    z_p = phases(hzp, COMPS, last[2])
    left = [jnp.where(lane == 0, pltpu.roll(z_m[j], 1, 1), pltpu.roll(own[j], 1, 1)) for j in range(2)]
    right = [
        jnp.where(lane == NZ - 1, pltpu.roll(z_p[j], NZ - 1, 1), pltpu.roll(own[j], NZ - 1, 1)) for j in range(2)
    ]
    in_l = jnp.where((lane == 0) & first[2], 0.0, 1.0)
    in_r = jnp.where((lane == NZ - 1) & last[2], 0.0, 1.0)
    in_x = [jnp.where(e[0], 0.0, 1.0) for e in (first, last)]
    in_y = [jnp.where(e[1], 0.0, 1.0) for e in (first, last)]
    tables = []
    for kind in range(2):
        pair = [lame_ref[p, 0] + (lame_ref[p, 0] + lame_ref[p, 1]) if kind else lame_ref[p, 0] for p in range(2)]

        def f(ph):
            return jnp.where(ph > 0.5, pair[1], pair[0])

        table = {}
        for j in range(2):
            here = f(own[j])
            table[XI + j] = here
            table[XLD + j] = 0.5 * (here + f(x_m[j]))
            table[XLO + j] = table[XLD + j] * in_x[0]
            table[XHD + j] = 0.5 * (here + f(x_p[j]))
            table[XHO + j] = table[XHD + j] * in_x[1]
            table[ZLD + j] = 0.5 * (here + f(left[j]))
            table[ZLO + j] = table[ZLD + j] * in_l
            table[ZRD + j] = 0.5 * (here + f(right[j]))
            table[ZRO + j] = table[ZRD + j] * in_r
        table[YM] = 0.5 * (f(own[0]) + f(own[1]))
        table[YLD] = 0.5 * (f(own[0]) + f(y_m[1]))
        table[YLO] = table[YLD] * in_y[0]
        table[YHD] = 0.5 * (f(own[1]) + f(y_p[0]))
        table[YHO] = table[YHD] * in_y[1]
        for row, value in table.items():
            w_ref[kind * KIND + row] = jnp.broadcast_to(value, (8, NZ))
        tables.append(table)
    for c in range(COMPS):
        tx, ty, tz = (tables[1 if c == d else 0] for d in range(3))
        for xc in range(3):
            for yc in range(6):
                j = yc // 3
                along_x = (tx[XLD + j] + tx[XI + j], tx[XI + j] + tx[XI + j], tx[XI + j] + tx[XHD + j])[xc]
                inner = ty[XI + j]
                along_y = (ty[YLD] + inner, inner + inner, inner + ty[YM], ty[YM] + inner, inner + inner, inner + ty[YHD])[yc]
                total = along_x + along_y + (tz[ZLD + j] + tz[ZRD + j])
                d_ref[(c * 3 + xc) * 6 + yc] = jnp.broadcast_to(total, (8, NZ))


def apply_operator(c, u_ref, halos, w_ref, d_ref, lane, done):
    hxm, hxp, hym, hyp, hzm, hzp = halos
    kx, ky, kz = (jnp.where(c == d, KIND, 0) for d in range(3))
    from_l = hzm[rows(c), :]
    from_r = hzp[rows(c), :]

    def at(xi, yi):
        start = (xi * NY + yi) * NZ
        return u_ref[c, :, start : start + NZ]

    def times(weight, value):
        return (weight[None] * value.reshape(4, 8, NZ)).reshape(VECS, NZ)

    for xi in range(NX):
        for yi in range(NY):
            j = yi // BRICK
            block = xi * NY + yi
            u = at(xi, yi)
            total = times(d_ref[(c * 3 + XCASE[xi]) * 6 + YCASE[yi]], u)
            if xi == 0:
                total -= times(w_ref[kx + XLO + j], hxm[rows(c * NY + yi), :])
            else:
                total -= times(w_ref[kx + XI + j], at(xi - 1, yi))
            if xi == NX - 1:
                total -= times(w_ref[kx + XHO + j], hxp[rows(c * NY + yi), :])
            else:
                total -= times(w_ref[kx + XI + j], at(xi + 1, yi))
            if yi == 0:
                total -= times(w_ref[ky + YLO], hym[rows(c * NX + xi), :])
            else:
                total -= times(w_ref[ky + (YM if yi == BRICK else XI + j)], at(xi, yi - 1))
            if yi == NY - 1:
                total -= times(w_ref[ky + YHO], hyp[rows(c * NX + xi), :])
            else:
                total -= times(w_ref[ky + (YM if yi == BRICK - 1 else XI + j)], at(xi, yi + 1))
            shift = (NZ - block) % NZ
            left = jnp.where(lane == 0, pltpu.roll(from_l, shift, 1) if shift else from_l, pltpu.roll(u, 1, 1))
            right = jnp.where(lane == NZ - 1, pltpu.roll(from_r, NZ - 1 - block, 1), pltpu.roll(u, NZ - 1, 1))
            total -= times(w_ref[kz + ZLO + j], left)
            total -= times(w_ref[kz + ZRO + j], right)
            done(xi, yi, total)


def step(u_ref, halos, w_ref, d_ref, v_ref, faces):
    lane = lanes()
    xl, xh, yl, yh, zl, zh = faces

    def comp(c, carry):
        ends = [jnp.zeros((VECS, NZ), F32), jnp.zeros((VECS, NZ), F32)]

        def done(xi, yi, value):
            start = (xi * NY + yi) * NZ
            v_ref[c, :, start : start + NZ] = value
            ends[:] = emit_faces(c, xi, yi, value, (xl, xh, yl, yh), ends[0], ends[1], lane)

        apply_operator(c, u_ref, halos, w_ref, d_ref, lane, done)
        zl[rows(c), :] = ends[0]
        zh[rows(c), :] = ends[1]
        return carry

    lax.fori_loop(0, COMPS, comp, 0)


def first_kernel(lame_ref, phase_ref, u_ref, hxm, hxp, hym, hyp, hzm, hzp, w_ref, d_ref, v_ref, xl, xh, yl, yh, zl, zh):
    halos = (hxm, hxp, hym, hyp, hzm, hzp)
    weight_tables(lame_ref, phase_ref, halos, w_ref, d_ref)
    step(u_ref, halos, w_ref, d_ref, v_ref, (xl, xh, yl, yh, zl, zh))


def next_kernel(w_ref, d_ref, u_ref, hxm, hxp, hym, hyp, hzm, hzp, v_ref, xl, xh, yl, yh, zl, zh):
    step(u_ref, (hxm, hxp, hym, hyp, hzm, hzp), w_ref, d_ref, v_ref, (xl, xh, yl, yh, zl, zh))


def gram_kernel(u_ref, g_ref):
    total = dot_t(u_ref[0], u_ref[0])
    for c in range(1, COMPS):
        total += dot_t(u_ref[c], u_ref[c])
    g_ref[...] = total


def cross_kernel(w_ref, d_ref, g1, g2, g3, u_ref, hxm, hxp, hym, hyp, hzm, hzp, out_ref, v_ref):
    lane = lanes()
    halos = (hxm, hxp, hym, hyp, hzm, hzp)

    def comp(c, total):
        def done(xi, yi, value):
            start = (xi * NY + yi) * NZ
            v_ref[:, start : start + NZ] = value

        apply_operator(c, u_ref, halos, w_ref, d_ref, lane, done)
        return total + dot_t(u_ref[c], v_ref[...])

    cross = lax.fori_loop(0, COMPS, comp, jnp.zeros((VECS, VECS), F32))
    out_ref[...] = jnp.concatenate([g1[...], g2[...], g3[...], cross], axis=1)


def inverse_factor(gram):
    row = lax.broadcasted_iota(jnp.int32, (VECS, VECS), 0)
    col = lax.broadcasted_iota(jnp.int32, (VECS, VECS), 1)
    work = jnp.concatenate([gram, jnp.where(row == col, 1.0, 0.0).astype(F32)], axis=1)
    below = lax.broadcasted_iota(jnp.int32, (VECS, 2 * VECS), 0)
    for k in range(VECS):
        pivot_row = work[k : k + 1, :]
        scale = lax.rsqrt(pivot_row[:, k : k + 1])
        scaled = pivot_row * scale
        factor = work[:, k : k + 1] * scale
        work = jnp.where(below == k, scaled, jnp.where(below > k, work - factor * scaled, work))
    return work[:, VECS:]


def final_kernel(n_rows, sums_ref, u_ref, basis_ref, coarse_ref):
    mixing = None
    for k in range(ITERS):
        gram = sums_ref[:, k * VECS : (k + 1) * VECS] / n_rows
        if mixing is not None:
            gram = dot_t(dot(mixing, gram), mixing)
        factor = inverse_factor(gram)
        mixing = factor if mixing is None else dot(factor, mixing)
    for c in range(COMPS):
        basis_ref[c] = dot(mixing, u_ref[c])
    coarse_ref[...] = dot_t(dot(mixing, sums_ref[:, ITERS * VECS :] / n_rows), mixing)


def face_shapes(extra):
    counts = (COMPS * NY,) * 2 + (COMPS * NX,) * 2 + (COMPS,) * 2
    return [pltpu.VMEM((n * VECS + extra, NZ), F32) for n in counts]


def exchange(faces):
    xl, xh, yl, yh, zl, zh = faces

    def ring(value, axis, by):
        n = lax.axis_size(axis)
        return lax.ppermute(value, axis, [(i, (i + by) % n) for i in range(n)])

    hzm, hzp = ring(zh, "gz", 1), ring(zl, "gz", -1)
    hxm, hxp = ring(xh, "gx", 1), ring(xl, "gx", -1)
    hym, hyp = ring(yh, "gy", 1), ring(yl, "gy", -1)
    return in_vmem(hxm, hxp, hym, hyp, hzm, hzp)


def all_sum(value):
    for axis, bits in (("gy", (1, 2)), ("gx", (1, 2)), ("gz", (1, 2, 4))):
        n = lax.axis_size(axis)
        for bit in bits:
            value = value + lax.ppermute(value, axis, [(i, i ^ bit) for i in range(n)])
    return value


def call(kernel, outs, ins, args, flops=4_000_000, scratch=()):
    return pl.pallas_call(
        kernel,
        out_shape=outs,
        in_specs=ins,
        out_specs=jax.tree.map(lambda _: VMEM, outs),
        scratch_shapes=scratch,
        cost_estimate=pl.CostEstimate(flops=flops, bytes_accessed=3_000_000, transcendentals=0),
        compiler_params=pltpu.CompilerParams(vmem_limit_bytes=24 * 1024 * 1024),
    )(*args)


def on_device(phase, lame, start):
    n_rows = 3.0 * start.shape[2] * start.shape[3] * start.shape[4]
    for axis in ("gx", "gy", "gz"):
        n_rows *= lax.axis_size(axis)
    field = pltpu.VMEM(FIELD, F32)
    (u,) = in_vmem(start.reshape(FIELD))
    faces = call(pack_kernel, face_shapes(8), [VMEM, VMEM], (u, phase))
    nodes = jnp.repeat(phase[0].astype(F32), BRICK, axis=1)
    nodes = jnp.concatenate([nodes, jnp.zeros((6, NZ), F32)])
    grams = []
    tables = None
    for k in range(ITERS):
        halos = exchange(faces)
        if tables is None:
            shapes = [pltpu.VMEM((2 * KIND, 8, NZ), F32), pltpu.VMEM((54, 8, NZ), F32), field] + face_shapes(0)
            w, d, u, *faces = call(first_kernel, shapes, [SMEM] + [VMEM] * 8, (lame, nodes, u, *halos))
            tables = (w, d)
        else:
            u, *faces = call(next_kernel, [field] + face_shapes(0), [VMEM] * 9, (*tables, u, *halos))
        u = in_vmem(u)[0]
        grams.append(call(gram_kernel, pltpu.VMEM((VECS, VECS), F32), [VMEM], (u,)))
    halos = exchange(faces)
    sums = call(
        cross_kernel,
        pltpu.VMEM((VECS, 4 * VECS), F32),
        [VMEM] * 12,
        (*tables, *grams, u, *halos),
        scratch=[pltpu.VMEM(FIELD[1:], F32)],
    )
    sums = all_sum(sums)
    basis, coarse = call(
        lambda *refs: final_kernel(n_rows, *refs),
        [field, jax.ShapeDtypeStruct((VECS, VECS), F32)],
        [VMEM, VMEM],
        (sums, u),
    )
    return basis.reshape(start.shape), coarse


def solution(mesh):
    in_specs = (P("gx", "gy", "gz"), P(), P(None, None, "gx", "gy", "gz"))
    out_specs = (P(None, None, "gx", "gy", "gz"), P())
    return jax.shard_map(on_device, mesh=mesh, in_specs=in_specs, out_specs=out_specs, check_vma=False)
```

```python
import jax
import jax.numpy as jnp
from jax import lax
from jax.experimental import pallas as pl
from jax.experimental.pallas import tpu as pltpu
from jax.sharding import PartitionSpec as P

ITERS = 3
BRICK = 4

COMPS, VECS, NX, NY, NZ = 3, 32, 4, 8, 128
FIELD = (COMPS, VECS, NX * NY * NZ)
F32 = jnp.float32

XI, XLD, XLO, XHD, XHO = 0, 2, 4, 6, 8
YM, YLD, YLO, YHD, YHO = 10, 11, 12, 13, 14
ZLD, ZLO, ZRD, ZRO = 15, 17, 19, 21
KIND = 23
YCASE = (0, 1, 1, 2, 3, 4, 4, 5)
XCASE = (0, 1, 1, 2)

VMEM = pl.BlockSpec(memory_space=pltpu.VMEM)
SMEM = pl.BlockSpec(memory_space=pltpu.SMEM)


def in_vmem(*arrays):
    return [pltpu.with_memory_space_constraint(a, pltpu.VMEM) for a in arrays]


def lanes():
    return lax.broadcasted_iota(jnp.int32, (VECS, NZ), 1)


def rows(block):
    return pl.ds(pl.multiple_of(block * VECS, VECS), VECS)


def dot_t(a, b):
    return lax.dot_general(
        a, b, (((1,), (1,)), ((), ())), precision=lax.Precision.HIGHEST, preferred_element_type=F32
    )


def dot(a, b):
    return jnp.dot(a, b, precision=lax.Precision.HIGHEST, preferred_element_type=F32)


def emit_faces(c, xi, yi, value, faces, last):
    half = NY // 2
    if not last:
        x_lo, x_hi, y_lo, y_hi = faces
        if xi == 0:
            x_lo[rows(c * NY + yi), :] = value
        if xi == NX - 1:
            x_hi[rows(c * NY + yi), :] = value
        if yi == 0:
            y_lo[rows(c * NX + xi), :] = value
    else:
        x_lo, x_hi, y_hi = faces
        if xi == 0 and yi >= half:
            x_lo[rows(c * half + yi - half), :] = value
        if xi == NX - 1 and yi < half:
            x_hi[rows(c * half + yi), :] = value
    if yi == NY - 1:
        y_hi[rows(c * NX + xi), :] = value


def emit_ends(v_ref, z_ref):
    lane = lanes()

    def comp(c, carry):
        ends = jnp.zeros((VECS, NZ), F32)
        for b in range(NX * NY):
            value = v_ref[c, :, b * NZ : (b + 1) * NZ]
            if b:
                value = pltpu.roll(value, 2 * b, 1)
            ends = jnp.where((lane == 2 * b) | (lane == (2 * b - 1) % NZ), value, ends)
        z_ref[rows(c), :] = ends
        return carry

    lax.fori_loop(0, COMPS, comp, 0)


def pack_kernel(u_ref, phase_ref, nodes_ref, xl, xh, yl, yh, ze):
    def comp(c, carry):
        for xi in range(NX):
            for yi in range(NY):
                if xi in (0, NX - 1) or yi in (0, NY - 1):
                    at = (xi * NY + yi) * NZ
                    emit_faces(c, xi, yi, u_ref[c, :, at : at + NZ], (xl, xh, yl, yh), False)
        return carry

    lax.fori_loop(0, COMPS, comp, 0)
    emit_ends(u_ref, ze)
    spread = (
        lax.broadcasted_iota(jnp.int32, (NZ // BRICK, NZ), 1) // BRICK
        == lax.broadcasted_iota(jnp.int32, (NZ // BRICK, NZ), 0)
    ).astype(F32)
    bricks = jnp.concatenate([phase_ref[0].astype(F32), jnp.zeros((6, NZ // BRICK), F32)], axis=0)
    nodes = jnp.dot(bricks, spread, preferred_element_type=F32)
    nodes_ref[...] = nodes
    for face, blocks in ((xl, COMPS * NY), (xh, COMPS * NY), (yl, COMPS * NX), (yh, COMPS * NX), (ze, COMPS)):
        face[blocks * VECS : blocks * VECS + 8, :] = nodes


def weight_tables(lame_ref, own_ref, halos, w_ref, d_ref):
    hxm, hxp, hym, hyp, hzm, hzp = halos
    lane = lax.broadcasted_iota(jnp.int32, (1, NZ), 1)
    first = [lax.axis_index(a) == 0 for a in ("gx", "gy", "gz")]
    last = [lax.axis_index(a) == lax.axis_size(a) - 1 for a in ("gx", "gy", "gz")]

    def phases(ref, blocks, outside):
        found = ref[blocks * VECS : blocks * VECS + 8, :]
        found = jnp.where(outside, 0.0, found)
        return [found[j : j + 1] for j in range(2)]

    own = own_ref[...]
    own = [own[j : j + 1] for j in range(2)]
    x_m = phases(hxm, COMPS * NY, first[0])
    x_p = phases(hxp, COMPS * NY, last[0])
    y_m = phases(hym, COMPS * NX, first[1])
    y_p = phases(hyp, COMPS * NX, last[1])
    z_m = phases(hzm, COMPS, first[2])
    z_p = phases(hzp, COMPS, last[2])
    left = [jnp.where(lane == 0, pltpu.roll(z_m[j], 1, 1), pltpu.roll(own[j], 1, 1)) for j in range(2)]
    right = [
        jnp.where(lane == NZ - 1, pltpu.roll(z_p[j], NZ - 1, 1), pltpu.roll(own[j], NZ - 1, 1)) for j in range(2)
    ]
    in_l = jnp.where((lane == 0) & first[2], 0.0, 1.0)
    in_r = jnp.where((lane == NZ - 1) & last[2], 0.0, 1.0)
    in_x = [jnp.where(e[0], 0.0, 1.0) for e in (first, last)]
    in_y = [jnp.where(e[1], 0.0, 1.0) for e in (first, last)]
    tables = []
    for kind in range(2):
        pair = [lame_ref[p, 0] + (lame_ref[p, 0] + lame_ref[p, 1]) if kind else lame_ref[p, 0] for p in range(2)]

        def f(ph):
            return jnp.where(ph > 0.5, pair[1], pair[0])

        table = {}
        for j in range(2):
            here = f(own[j])
            table[XI + j] = here
            table[XLD + j] = 0.5 * (here + f(x_m[j]))
            table[XLO + j] = table[XLD + j] * in_x[0]
            table[XHD + j] = 0.5 * (here + f(x_p[j]))
            table[XHO + j] = table[XHD + j] * in_x[1]
            table[ZLD + j] = 0.5 * (here + f(left[j]))
            table[ZLO + j] = table[ZLD + j] * in_l
            table[ZRD + j] = 0.5 * (here + f(right[j]))
            table[ZRO + j] = table[ZRD + j] * in_r
        table[YM] = 0.5 * (f(own[0]) + f(own[1]))
        table[YLD] = 0.5 * (f(own[0]) + f(y_m[1]))
        table[YLO] = table[YLD] * in_y[0]
        table[YHD] = 0.5 * (f(own[1]) + f(y_p[0]))
        table[YHO] = table[YHD] * in_y[1]
        for row, value in table.items():
            w_ref[kind * KIND + row] = jnp.broadcast_to(value, (8, NZ))
        tables.append(table)
    for c in range(COMPS):
        tx, ty, tz = (tables[1 if c == d else 0] for d in range(3))
        for xc in range(3):
            for yc in range(6):
                j = yc // 3
                along_x = (tx[XLD + j] + tx[XI + j], tx[XI + j] + tx[XI + j], tx[XI + j] + tx[XHD + j])[xc]
                inner = ty[XI + j]
                along_y = (ty[YLD] + inner, inner + inner, inner + ty[YM], ty[YM] + inner, inner + inner, inner + ty[YHD])[yc]
                total = along_x + along_y + (tz[ZLD + j] + tz[ZRD + j])
                d_ref[(c * 3 + xc) * 6 + yc] = jnp.broadcast_to(total, (8, NZ))


def apply_operator(c, u_ref, halos, w_ref, d_ref, done, last=False):
    lane = lanes()
    kx, ky, kz = (jnp.where(c == d, KIND, 0) for d in range(3))
    half = NY // 2
    if last:
        hxm, hxp, hym, hzm = halos
        ends = jnp.where(lane % 2 == 0, 0.0, pltpu.roll(2.0 * hzm[rows(c), :], 2, 1))
    else:
        hxm, hxp, hym, hyp, hzm, hzp = halos
        ends = jnp.where(lane % 2 == 0, hzp[rows(c), :], pltpu.roll(hzm[rows(c), :], 2, 1))

    def at(xi, yi):
        start = (xi * NY + yi) * NZ
        return u_ref[c, :, start : start + NZ]

    def times(weight, value):
        return (weight[None] * value.reshape(4, 8, NZ)).reshape(VECS, NZ)

    for xi in range(NX):
        for yi in range(NY):
            j = yi // BRICK
            block = xi * NY + yi
            u = at(xi, yi)
            total = times(d_ref[(c * 3 + XCASE[xi]) * 6 + YCASE[yi]], u)
            if xi > 0:
                total -= times(w_ref[kx + XI + j], at(xi - 1, yi))
            elif not last:
                total -= times(w_ref[kx + XLO + j], hxm[rows(c * NY + yi), :])
            elif yi < half:
                total -= times(2.0 * w_ref[kx + XLO + j], hxm[rows(c * half + yi), :])
            if xi < NX - 1:
                total -= times(w_ref[kx + XI + j], at(xi + 1, yi))
            elif not last:
                total -= times(w_ref[kx + XHO + j], hxp[rows(c * NY + yi), :])
            elif yi >= half:
                total -= times(2.0 * w_ref[kx + XHO + j], hxp[rows(c * half + yi - half), :])
            if yi > 0:
                total -= times(w_ref[ky + (YM if yi == BRICK else XI + j)], at(xi, yi - 1))
            else:
                weight = w_ref[ky + YLO]
                total -= times(2.0 * weight if last else weight, hym[rows(c * NX + xi), :])
            if yi < NY - 1:
                total -= times(w_ref[ky + (YM if yi == BRICK - 1 else XI + j)], at(xi, yi + 1))
            elif not last:
                total -= times(w_ref[ky + YHO], hyp[rows(c * NX + xi), :])
            outer = pltpu.roll(ends, NZ - 1 - 2 * block, 1)
            left = jnp.where(lane == 0, outer, pltpu.roll(u, 1, 1))
            right = jnp.where(lane == NZ - 1, outer, pltpu.roll(u, NZ - 1, 1))
            total -= times(w_ref[kz + ZLO + j], left)
            total -= times(w_ref[kz + ZRO + j], right)
            done(xi, yi, total)


def step(u_ref, halos, w_ref, d_ref, v_ref, faces, ends_ref, last):
    def comp(c, carry):
        def done(xi, yi, value):
            start = (xi * NY + yi) * NZ
            v_ref[c, :, start : start + NZ] = value
            emit_faces(c, xi, yi, value, faces, last)

        apply_operator(c, u_ref, halos, w_ref, d_ref, done)
        return carry

    lax.fori_loop(0, COMPS, comp, 0)
    emit_ends(v_ref, ends_ref)


def first_kernel(lame_ref, nodes_ref, u_ref, hxm, hxp, hym, hyp, hzm, hzp, w_ref, d_ref, v_ref, *faces):
    halos = (hxm, hxp, hym, hyp, hzm, hzp)
    weight_tables(lame_ref, nodes_ref, halos, w_ref, d_ref)
    step(u_ref, halos, w_ref, d_ref, v_ref, faces[:-1], faces[-1], False)


def middle_kernel(w_ref, d_ref, u_ref, hxm, hxp, hym, hyp, hzm, hzp, v_ref, *faces):
    step(u_ref, (hxm, hxp, hym, hyp, hzm, hzp), w_ref, d_ref, v_ref, faces[:-1], faces[-1], False)


def third_kernel(w_ref, d_ref, u_ref, hxm, hxp, hym, hyp, hzm, hzp, v_ref, *faces):
    step(u_ref, (hxm, hxp, hym, hyp, hzm, hzp), w_ref, d_ref, v_ref, faces[:-1], faces[-1], True)


def gram_kernel(u_ref, g_ref):
    total = dot_t(u_ref[0], u_ref[0])
    for c in range(1, COMPS):
        total += dot_t(u_ref[c], u_ref[c])
    g_ref[...] = total


def cross_kernel(w_ref, d_ref, g1, g2, g3, u_ref, hxm, hxp, hym, hzm, out_ref, v_ref):
    halos = (hxm, hxp, hym, hzm)

    def comp(c, total):
        def done(xi, yi, value):
            start = (xi * NY + yi) * NZ
            v_ref[:, start : start + NZ] = value

        apply_operator(c, u_ref, halos, w_ref, d_ref, done, last=True)
        return total + dot_t(u_ref[c], v_ref[...])

    cross = lax.fori_loop(0, COMPS, comp, jnp.zeros((VECS, VECS), F32))
    out_ref[...] = jnp.concatenate([g1[...], g2[...], g3[...], cross], axis=1)


def inverse_factor(gram):
    row = lax.broadcasted_iota(jnp.int32, (8, NZ), 0)
    col = lax.broadcasted_iota(jnp.int32, (8, NZ), 1)
    groups = VECS // 8
    cols = []
    for k in range(VECS):
        whole = jnp.broadcast_to(gram[:, k : k + 1], (VECS, NZ))
        cols.append([whole[8 * g : 8 * g + 8] for g in range(groups)])
    unit = [jnp.where(row + 8 * g == col, 1.0, 0.0).astype(F32) for g in range(groups)]

    def spread(group, r):
        return jnp.broadcast_to(group[r : r + 1], (8, NZ))

    for k in range(VECS):
        own, r = divmod(k, 8)
        scale = lax.rsqrt(spread(cols[k][own], r))
        factor = [None] * own + [cols[k][g] * scale for g in range(own, groups)]
        pivot = spread(unit[own], r) * scale
        for j in range(k + 1, VECS):
            at_j = spread(factor[j // 8], j % 8)
            for g in range(j // 8, groups):
                cols[j][g] = cols[j][g] - factor[g] * at_j
        unit[own] = jnp.where(row == r, pivot, jnp.where(row > r, unit[own] - factor[own] * pivot, unit[own]))
        for g in range(own + 1, groups):
            unit[g] = unit[g] - factor[g] * pivot
    return jnp.concatenate(unit, axis=0)[:, :VECS]


def factor_kernel(n_rows, sums_ref, mixing_ref, coarse_ref, grams_ref, turned_ref):
    for k in range(ITERS):
        grams_ref[k] = sums_ref[:, k * VECS : (k + 1) * VECS] / n_rows
    cross = sums_ref[:, ITERS * VECS :] / n_rows
    turned_ref[...] = cross.T
    grams_ref[ITERS] = 0.5 * (cross + turned_ref[...])

    def congruent(k, mixing):
        turned_ref[...] = mixing.T
        return dot(dot(mixing, grams_ref[k]), turned_ref[...])

    mixing = inverse_factor(grams_ref[0])
    for k in range(1, ITERS):
        mixing = dot(inverse_factor(congruent(k, mixing)), mixing)
    coarse_ref[...] = congruent(ITERS, mixing)
    mixing_ref[...] = mixing


def basis_kernel(mixing_ref, u_ref, basis_ref):
    for c in range(COMPS):
        basis_ref[c] = dot(mixing_ref[...], u_ref[c])


def face_shapes(extra=0, last=False):
    counts = (COMPS * NY,) * 2 + (COMPS * NX,) * 2 + (COMPS,)
    if last:
        counts = (COMPS * NY // 2,) * 2 + (COMPS * NX, COMPS)
    return [pltpu.VMEM((n * VECS + extra, NZ), F32) for n in counts]


def ring(value, axis, by):
    n = lax.axis_size(axis)
    return lax.ppermute(value, axis, [(i, (i + by) % n) for i in range(n)])


def exchange(xl, xh, yl, yh, ze):
    return in_vmem(
        ring(xh, "gx", 1), ring(xl, "gx", -1), ring(yh, "gy", 1), ring(yl, "gy", -1), ring(ze, "gz", 1), ring(ze, "gz", -1)
    )


def last_exchange(xl, xh, yh, ze):
    return in_vmem(ring(xh, "gx", 1), ring(xl, "gx", -1), ring(yh, "gy", 1), ring(ze, "gz", 1))


def all_sum(value):
    value = value + lax.ppermute(value, "gy", [(i, i ^ 1) for i in range(4)])

    def along_x(by):
        pairs = []
        for i in range(32):
            x_low, core, x_high, z = i // 16, i // 8 % 2, i // 4 % 2, i % 4
            x = (2 * x_high + x_low + by) % 4
            pairs.append((i, (x % 2) * 16 + core * 8 + (x // 2) * 4 + z))
        return pairs

    def along_z(by):
        return [(i, i // 4 * 4 + (i % 4 + by) % 4) for i in range(8)]

    def along_y(by):
        return [(i, (i + by) % 4) for i in range(4)]

    for axis, pairs in ((("gy", "gz"), along_x), ("gx", along_y), ("gz", along_z)):
        one, three, two = (lax.ppermute(value, axis, pairs(by)) for by in (1, 3, 2))
        value = (value + two) + (one + three)
    return value


def call(kernel, outs, ins, args, flops=4_000_000, scratch=()):
    return pl.pallas_call(
        kernel,
        out_shape=outs,
        in_specs=ins,
        out_specs=jax.tree.map(lambda _: VMEM, outs),
        scratch_shapes=scratch,
        cost_estimate=pl.CostEstimate(flops=flops, bytes_accessed=3_000_000, transcendentals=0),
        compiler_params=pltpu.CompilerParams(vmem_limit_bytes=24 * 1024 * 1024),
    )(*args)


def gram_of(u):
    return call(gram_kernel, pltpu.VMEM((VECS, VECS), F32), [VMEM], (u,))


def on_device(phase, lame, start):
    n_rows = 3.0 * start.shape[2] * start.shape[3] * start.shape[4]
    for axis in ("gx", "gy", "gz"):
        n_rows *= lax.axis_size(axis)
    field = pltpu.VMEM(FIELD, F32)
    (u,) = in_vmem(start.reshape(FIELD))
    nodes, *faces = call(pack_kernel, [pltpu.VMEM((8, NZ), F32)] + face_shapes(8), [VMEM, VMEM], (u, phase))
    halos = exchange(*faces)
    shapes = [pltpu.VMEM((2 * KIND, 8, NZ), F32), pltpu.VMEM((54, 8, NZ), F32), field] + face_shapes()
    w, d, u, *faces = call(first_kernel, shapes, [SMEM] + [VMEM] * 8, (lame, nodes, u, *halos))
    grams = [gram_of(u)]
    halos = exchange(*faces)
    u, *faces = call(middle_kernel, [field] + face_shapes(), [VMEM] * 9, (w, d, u, *halos))
    grams.append(gram_of(u))
    halos = exchange(*faces)
    u, *faces = call(third_kernel, [field] + face_shapes(last=True), [VMEM] * 9, (w, d, u, *halos))
    grams.append(gram_of(u))
    halos = last_exchange(*faces)
    sums = call(
        cross_kernel,
        pltpu.VMEM((VECS, 4 * VECS), F32),
        [VMEM] * 10,
        (w, d, *grams, u, *halos),
        scratch=[pltpu.VMEM(FIELD[1:], F32)],
    )
    small = jax.ShapeDtypeStruct((VECS, VECS), F32)
    mixing, coarse = call(
        lambda *refs: factor_kernel(n_rows, *refs),
        [pltpu.VMEM((VECS, VECS), F32), small],
        [VMEM],
        (all_sum(sums),),
        scratch=[pltpu.VMEM((ITERS + 1, VECS, VECS), F32), pltpu.VMEM((VECS, VECS), F32)],
    )
    basis = call(basis_kernel, field, [VMEM, VMEM], (mixing, u))
    return basis.reshape(start.shape), coarse


def solution(mesh):
    in_specs = (P("gx", "gy", "gz"), P(), P(None, None, "gx", "gy", "gz"))
    out_specs = (P(None, None, "gx", "gy", "gz"), P())
    return jax.shard_map(on_device, mesh=mesh, in_specs=in_specs, out_specs=out_specs, check_vma=False)
```

```python
import functools

import jax
import jax.numpy as jnp
from jax import lax
from jax.experimental import pallas as pl
from jax.experimental.pallas import tpu as pltpu
from jax.sharding import PartitionSpec as P


ITERS = 3
BRICK = 4

COMPS, VECS, NX, NY, NZ = 3, 32, 4, 8, 128
HALF = (COMPS, VECS, NX * NY * NZ // 2)
OUTER, INNER = (0, NX - 1), (1, NX - 2)
F32 = jnp.float32

XI, XLD, XLO, XHD, XHO = 0, 2, 4, 6, 8
YM, YLD, YLO, YHD, YHO = 10, 11, 12, 13, 14
ZLD, ZLO, ZRD, ZRO = 15, 17, 19, 21
KIND = 23
LIMIT = 24 * 1024 * 1024
YCASE = (0, 1, 1, 2, 3, 4, 4, 5)
XCASE = (0, 1, 1, 2)

VMEM = pl.BlockSpec(memory_space=pltpu.VMEM)
SMEM = pl.BlockSpec(memory_space=pltpu.SMEM)


def in_vmem(*arrays):
    return [pltpu.with_memory_space_constraint(a, pltpu.VMEM) for a in arrays]


def lanes():
    return lax.broadcasted_iota(jnp.int32, (VECS, NZ), 1)


def rows(block):
    return pl.ds(pl.multiple_of(block * VECS, VECS), VECS)


def dot_t(a, b):
    return lax.dot_general(
        a, b, (((1,), (1,)), ((), ())), precision=lax.Precision.HIGHEST, preferred_element_type=F32
    )


def dot(a, b):
    return jnp.dot(a, b, precision=lax.Precision.HIGHEST, preferred_element_type=F32)


def block_of(outer, inner, c, xi, yi):
    ref = outer if xi in OUTER else inner
    start = ((xi > 1) * NY + yi) * NZ
    return ref.at[c, :, pl.ds(start, NZ)]


def emit_x(c, xi, yi, value, faces, last):
    x_lo, x_hi = faces
    half = NY // 2
    if not last:
        (x_lo if xi == 0 else x_hi)[rows(c * NY + yi), :] = value
    elif xi == 0 and yi >= half:
        x_lo[rows(c * half + yi - half), :] = value
    elif xi > 0 and yi < half:
        x_hi[rows(c * half + yi), :] = value


def emit_y_z(outer, inner, faces, last):
    lane = lanes()

    def comp(c, carry):
        ends = jnp.zeros((VECS, NZ), F32)
        for xi in range(NX):
            for yi in range(NY):
                value = block_of(outer, inner, c, xi, yi)[...]
                if yi == 0 and not last:
                    faces[1][rows(c * NX + xi), :] = value
                if yi == NY - 1:
                    faces[0][rows(c * NX + xi), :] = value
                b = xi * NY + yi
                if b:
                    value = pltpu.roll(value, 2 * b, 1)
                ends = jnp.where((lane == 2 * b) | (lane == (2 * b - 1) % NZ), value, ends)
        faces[-1][rows(c), :] = ends
        return carry

    lax.fori_loop(0, COMPS, comp, 0)


def node_phases(phase_ref):
    spread = (
        lax.broadcasted_iota(jnp.int32, (NZ // BRICK, NZ), 1) // BRICK
        == lax.broadcasted_iota(jnp.int32, (NZ // BRICK, NZ), 0)
    ).astype(F32)
    bricks = jnp.concatenate([phase_ref[0].astype(F32), jnp.zeros((6, NZ // BRICK), F32)], axis=0)
    return jnp.dot(bricks, spread, preferred_element_type=F32)


def native(xi, yi):
    return pl.ds(xi * NY + yi, VECS, stride=NX * NY)


def pack_outer_kernel(x_ref, phase_ref, nodes_ref, outer, x_lo, x_hi):
    for c in range(COMPS):
        for xi in OUTER:
            for yi in range(NY):
                value = x_ref[pl.ds(c * NX * NY * VECS + xi * NY + yi, VECS, stride=NX * NY), :]
                block_of(outer, None, c, xi, yi)[...] = value
                emit_x(c, xi, yi, value, (x_lo, x_hi), False)
    nodes = node_phases(phase_ref)
    nodes_ref[...] = nodes
    for face in (x_lo, x_hi):
        face[COMPS * NY * VECS : COMPS * NY * VECS + 8, :] = nodes


def pack_inner_kernel(x_ref, nodes_ref, outer, inner, y_hi, y_lo, ends):
    for c in range(COMPS):
        for xi in INNER:
            for yi in range(NY):
                value = x_ref[pl.ds(c * NX * NY * VECS + xi * NY + yi, VECS, stride=NX * NY), :]
                block_of(outer, inner, c, xi, yi)[...] = value
    emit_y_z(outer, inner, (y_hi, y_lo, ends), False)
    for face, blocks in ((y_hi, COMPS * NX), (y_lo, COMPS * NX), (ends, COMPS)):
        face[blocks * VECS : blocks * VECS + 8, :] = nodes_ref[...]


def weight_tables(lame_ref, own_ref, halos, w_ref, d_ref):
    hxm, hxp, hym, hyp, hzm, hzp = halos
    lane = lax.broadcasted_iota(jnp.int32, (1, NZ), 1)
    first = [lax.axis_index(a) == 0 for a in ("gx", "gy", "gz")]
    last = [lax.axis_index(a) == lax.axis_size(a) - 1 for a in ("gx", "gy", "gz")]

    def phases(ref, blocks, outside):
        found = ref[blocks * VECS : blocks * VECS + 8, :]
        found = jnp.where(outside, 0.0, found)
        return [found[j : j + 1] for j in range(2)]

    own = own_ref[...]
    own = [own[j : j + 1] for j in range(2)]
    x_m = phases(hxm, COMPS * NY, first[0])
    x_p = phases(hxp, COMPS * NY, last[0])
    y_m = phases(hym, COMPS * NX, first[1])
    y_p = phases(hyp, COMPS * NX, last[1])
    z_m = phases(hzm, COMPS, first[2])
    z_p = phases(hzp, COMPS, last[2])
    left = [jnp.where(lane == 0, pltpu.roll(z_m[j], 1, 1), pltpu.roll(own[j], 1, 1)) for j in range(2)]
    right = [
        jnp.where(lane == NZ - 1, pltpu.roll(z_p[j], NZ - 1, 1), pltpu.roll(own[j], NZ - 1, 1)) for j in range(2)
    ]
    in_l = jnp.where((lane == 0) & first[2], 0.0, 1.0)
    in_r = jnp.where((lane == NZ - 1) & last[2], 0.0, 1.0)
    in_x = [jnp.where(e[0], 0.0, 1.0) for e in (first, last)]
    in_y = [jnp.where(e[1], 0.0, 1.0) for e in (first, last)]
    tables = []
    for kind in range(2):
        pair = [lame_ref[p, 0] + (lame_ref[p, 0] + lame_ref[p, 1]) if kind else lame_ref[p, 0] for p in range(2)]

        def f(ph):
            return jnp.where(ph > 0.5, pair[1], pair[0])

        table = {}
        for j in range(2):
            here = f(own[j])
            table[XI + j] = here
            table[XLD + j] = 0.5 * (here + f(x_m[j]))
            table[XLO + j] = table[XLD + j] * in_x[0]
            table[XHD + j] = 0.5 * (here + f(x_p[j]))
            table[XHO + j] = table[XHD + j] * in_x[1]
            table[ZLD + j] = 0.5 * (here + f(left[j]))
            table[ZLO + j] = table[ZLD + j] * in_l
            table[ZRD + j] = 0.5 * (here + f(right[j]))
            table[ZRO + j] = table[ZRD + j] * in_r
        table[YM] = 0.5 * (f(own[0]) + f(own[1]))
        table[YLD] = 0.5 * (f(own[0]) + f(y_m[1]))
        table[YLO] = table[YLD] * in_y[0]
        table[YHD] = 0.5 * (f(own[1]) + f(y_p[0]))
        table[YHO] = table[YHD] * in_y[1]
        for row, value in table.items():
            w_ref[kind * KIND + row] = jnp.broadcast_to(value, (8, NZ))
        tables.append(table)
    for c in range(COMPS):
        tx, ty, tz = (tables[1 if c == d else 0] for d in range(3))
        for xc in range(3):
            for yc in range(6):
                j = yc // 3
                along_x = (tx[XLD + j] + tx[XI + j], tx[XI + j] + tx[XI + j], tx[XI + j] + tx[XHD + j])[xc]
                inner = ty[XI + j]
                along_y = (ty[YLD] + inner, inner + inner, inner + ty[YM], ty[YM] + inner, inner + inner, inner + ty[YHD])[yc]
                total = along_x + along_y + (tz[ZLD + j] + tz[ZRD + j])
                d_ref[(c * 3 + xc) * 6 + yc] = jnp.broadcast_to(total, (8, NZ))


def times(weight, value):
    return (weight[None] * value.reshape(4, 8, NZ)).reshape(VECS, NZ)


def kinds(c):
    return [jnp.where(c == d, KIND, 0) for d in range(3)]


def apply_operator(c, outer, inner, halos, w_ref, d_ref, layers, done):
    lane = lanes()
    kx, ky, kz = kinds(c)
    if halos:
        hxm, hxp, hym, hyp, hzm, hzp = halos
        ends = jnp.where(lane % 2 == 0, hzp[rows(c), :], pltpu.roll(hzm[rows(c), :], 2, 1))

    def at(xi, yi):
        return block_of(outer, inner, c, xi, yi)[...]

    for xi in layers:
        for yi in range(NY):
            j = yi // BRICK
            block = xi * NY + yi
            u = at(xi, yi)
            total = times(d_ref[(c * 3 + XCASE[xi]) * 6 + YCASE[yi]], u)
            if xi > 0:
                total -= times(w_ref[kx + XI + j], at(xi - 1, yi))
            elif halos:
                total -= times(w_ref[kx + XLO + j], hxm[rows(c * NY + yi), :])
            if xi < NX - 1:
                total -= times(w_ref[kx + XI + j], at(xi + 1, yi))
            elif halos:
                total -= times(w_ref[kx + XHO + j], hxp[rows(c * NY + yi), :])
            if yi > 0:
                total -= times(w_ref[ky + (YM if yi == BRICK else XI + j)], at(xi, yi - 1))
            elif halos:
                total -= times(w_ref[ky + YLO], hym[rows(c * NX + xi), :])
            if yi < NY - 1:
                total -= times(w_ref[ky + (YM if yi == BRICK - 1 else XI + j)], at(xi, yi + 1))
            elif halos:
                total -= times(w_ref[ky + YHO], hyp[rows(c * NX + xi), :])
            left, right = pltpu.roll(u, 1, 1), pltpu.roll(u, NZ - 1, 1)
            if halos:
                far = pltpu.roll(ends, NZ - 1 - 2 * block, 1)
                left, right = jnp.where(lane == 0, far, left), jnp.where(lane == NZ - 1, far, right)
            else:
                left, right = jnp.where(lane == 0, 0.0, left), jnp.where(lane == NZ - 1, 0.0, right)
            total -= times(w_ref[kz + ZLO + j], left)
            total -= times(w_ref[kz + ZRO + j], right)
            done(xi, yi, total)


def outer_step(w_ref, d_ref, refs, last):
    outer, inner, hxm, hxp, hym, hyp, hzm, hzp, new_outer, x_lo, x_hi = refs

    def comp(c, carry):
        def done(xi, yi, value):
            block_of(new_outer, None, c, xi, yi)[...] = value
            emit_x(c, xi, yi, value, (x_lo, x_hi), last)

        apply_operator(c, outer, inner, (hxm, hxp, hym, hyp, hzm, hzp), w_ref, d_ref, OUTER, done)
        return carry

    lax.fori_loop(0, COMPS, comp, 0)


def first_outer_kernel(lame_ref, nodes_ref, *refs):
    w_ref, d_ref = refs[8:10]
    weight_tables(lame_ref, nodes_ref, refs[2:8], w_ref, d_ref)
    outer_step(w_ref, d_ref, refs[:8] + refs[10:], False)


def outer_kernel(last, w_ref, d_ref, *refs):
    outer_step(w_ref, d_ref, refs, last)


def inner_kernel(last, w_ref, d_ref, outer, inner, hym, hyp, hzm, hzp, new_outer, new_inner, *faces):
    def comp(c, carry):
        def done(xi, yi, value):
            block_of(None, new_inner, c, xi, yi)[...] = value

        apply_operator(c, outer, inner, (None, None, hym, hyp, hzm, hzp), w_ref, d_ref, INNER, done)
        return carry

    lax.fori_loop(0, COMPS, comp, 0)
    emit_y_z(new_outer, new_inner, faces, last)


def gram_kernel(outer, inner, g_ref):
    total = jnp.zeros((VECS, VECS), F32)
    for ref in (outer, inner):
        for c in range(COMPS):
            total += dot_t(ref[c], ref[c])
    g_ref[...] = total


def inside_kernel(w_ref, d_ref, outer, inner, out_ref, pair_ref):
    def comp(c, total):
        def done(xi, yi, value):
            start = (xi * NY + yi) * NZ
            pair_ref[VECS:, start : start + NZ] = value

        apply_operator(c, outer, inner, None, w_ref, d_ref, range(NX), done)
        for xi in range(NX):
            ref, start = (outer if xi in OUTER else inner), (xi > 1) * NY * NZ
            pair_ref[:VECS, xi * NY * NZ : (xi + 1) * NY * NZ] = ref[c, :, start : start + NY * NZ]
        return total + dot_t(pair_ref[:VECS, :], pair_ref[...])

    out_ref[...] = lax.fori_loop(0, COMPS, comp, jnp.zeros((VECS, 2 * VECS), F32))


def across_kernel(w_ref, g1, g2, inside, outer, inner, own_ends, hxm, hxp, hym, hzm, out_ref):
    lane = lanes()
    half = NY // 2

    def comp(c, total):
        kx, ky, kz = kinds(c)
        mine, other = [], []
        for yi in range(NY):
            j = yi // BRICK
            xi = 0 if yi < half else NX - 1
            mine.append(block_of(outer, inner, c, xi, yi)[...])
            halo = hxm if yi < half else hxp
            other.append(times(w_ref[kx + (XLO if yi < half else XHO) + j], halo[rows(c * half + yi % half), :]))
        for xi in range(NX):
            mine.append(block_of(outer, inner, c, xi, 0)[...])
            other.append(times(w_ref[ky + YLO], hym[rows(c * NX + xi), :]))
        weight = [jnp.broadcast_to(w_ref[kz + ZLO + j][:, :1], (8, NZ)) for j in range(2)]
        which = lax.broadcasted_iota(jnp.int32, (8, NZ), 1)
        weight = jnp.where(which // 2 % NY < BRICK, weight[0], weight[1])
        weight = jnp.where((which % 2 == 0) & (which < 2 * NX * NY), weight, 0.0)
        mine.append(own_ends[rows(c), :])
        other.append(times(weight, pltpu.roll(hzm[rows(c), :], 1, 1)))
        return total + dot_t(jnp.concatenate(mine, axis=1), jnp.concatenate(other, axis=1))

    cross = lax.fori_loop(0, COMPS, comp, jnp.zeros((VECS, VECS), F32))
    both = inside[...]
    out_ref[...] = jnp.concatenate([g1[...], g2[...], both[:, :VECS], both[:, VECS:] - 2.0 * cross], axis=1)


def inverse_factor(gram):
    row = lax.broadcasted_iota(jnp.int32, (8, NZ), 0)
    col = lax.broadcasted_iota(jnp.int32, (8, NZ), 1)
    groups = VECS // 8
    cols = []
    for k in range(VECS):
        whole = jnp.broadcast_to(gram[:, k : k + 1], (VECS, NZ))
        cols.append([whole[8 * g : 8 * g + 8] for g in range(groups)])
    unit = [jnp.where(row + 8 * g == col, 1.0, 0.0).astype(F32) for g in range(groups)]

    def spread(group, r):
        return jnp.broadcast_to(group[r : r + 1], (8, NZ))

    for k in range(VECS):
        own, r = divmod(k, 8)
        scale = lax.rsqrt(spread(cols[k][own], r))
        factor = [None] * own + [cols[k][g] * scale for g in range(own, groups)]
        pivot = spread(unit[own], r) * scale
        for j in range(k + 1, VECS):
            at_j = spread(factor[j // 8], j % 8)
            for g in range(j // 8, groups):
                cols[j][g] = cols[j][g] - factor[g] * at_j
        unit[own] = jnp.where(row == r, pivot, jnp.where(row > r, unit[own] - factor[own] * pivot, unit[own]))
        for g in range(own + 1, groups):
            unit[g] = unit[g] - factor[g] * pivot
    return jnp.concatenate(unit, axis=0)[:, :VECS]


def factor_kernel(n_rows, sums_ref, mixing_ref, coarse_ref, grams_ref, turned_ref):
    for k in range(ITERS):
        grams_ref[k] = sums_ref[:, k * VECS : (k + 1) * VECS] / n_rows
    cross = sums_ref[:, ITERS * VECS :] / n_rows
    turned_ref[...] = cross.T
    grams_ref[ITERS] = 0.5 * (cross + turned_ref[...])

    def congruent(k, mixing):
        turned_ref[...] = mixing.T
        return dot(dot(mixing, grams_ref[k]), turned_ref[...])

    mixing = inverse_factor(grams_ref[0])
    for k in range(1, ITERS):
        mixing = dot(inverse_factor(congruent(k, mixing)), mixing)
    coarse_ref[...] = congruent(ITERS, mixing)
    mixing_ref[...] = mixing


def basis_kernel(mixing_ref, outer, inner, basis_ref):
    c = pl.program_id(0)
    for half, layers in ((outer, OUTER), (inner, INNER)):
        value = dot(mixing_ref[...], half[c])
        for slot, xi in enumerate(layers):
            for yi in range(NY):
                start = (slot * NY + yi) * NZ
                basis_ref[native(xi, yi), :] = value[:, start : start + NZ]


def vmem(*shape):
    return pltpu.VMEM(shape, F32)


def faces_x(extra=0, last=False):
    return [vmem(COMPS * NY * VECS // (2 if last else 1) + extra, NZ)] * 2


def faces_y_z(extra=0, last=False):
    return [vmem(COMPS * NX * VECS + extra, NZ)] * (1 if last else 2) + [vmem(COMPS * VECS + extra, NZ)]


def ring(value, axis, by):
    n = lax.axis_size(axis)
    return lax.ppermute(value, axis, [(i, (i + by) % n) for i in range(n)])


def send_x(x_lo, x_hi):
    return in_vmem(ring(x_hi, "gx", 1), ring(x_lo, "gx", -1))


def send_y_z(y_hi, y_lo, ends):
    return in_vmem(ring(y_hi, "gy", 1), ring(y_lo, "gy", -1), ring(ends, "gz", 1), ring(ends, "gz", -1))


def all_sum(value):
    value = value + lax.ppermute(value, "gy", [(i, i ^ 1) for i in range(4)])

    def along_x(by):
        pairs = []
        for i in range(32):
            x_low, core, x_high, z = i // 16, i // 8 % 2, i // 4 % 2, i % 4
            x = (2 * x_high + x_low + by) % 4
            pairs.append((i, (x % 2) * 16 + core * 8 + (x // 2) * 4 + z))
        return pairs

    def along_z(by):
        return [(i, i // 4 * 4 + (i % 4 + by) % 4) for i in range(8)]

    def along_y(by):
        return [(i, (i + by) % 4) for i in range(4)]

    for axis, pairs in ((("gy", "gz"), along_x), ("gx", along_y), ("gz", along_z)):
        one, three, two = (lax.ppermute(value, axis, pairs(by)) for by in (1, 3, 2))
        value = (value + two) + (one + three)
    return value


def call(kernel, outs, args, flops=4_000_000, scratch=(), smem=0):
    return pl.pallas_call(
        kernel,
        out_shape=outs,
        in_specs=[SMEM] * smem + [VMEM] * (len(args) - smem),
        out_specs=jax.tree.map(lambda _: VMEM, outs),
        scratch_shapes=scratch,
        cost_estimate=pl.CostEstimate(flops=flops, bytes_accessed=3_000_000, transcendentals=0),
        compiler_params=pltpu.CompilerParams(vmem_limit_bytes=LIMIT),
    )(*args)


def on_device(phase, lame, start):
    n_rows = 3.0 * start.shape[2] * start.shape[3] * start.shape[4]
    for axis in ("gx", "gy", "gz"):
        n_rows *= lax.axis_size(axis)
    field, small = vmem(*HALF), vmem(VECS, VECS)
    (flat,) = in_vmem(start.reshape(-1, NZ))
    grams = []
    for k in range(ITERS + 1):
        last = k == ITERS
        if k == 0:
            nodes, outer, *x_faces = call(pack_outer_kernel, [vmem(8, NZ), field] + faces_x(8), (flat, phase))
        elif k == 1:
            tables = [vmem(2 * KIND, 8, NZ), vmem(54, 8, NZ)]
            w, d, new_outer, *x_faces = call(
                first_outer_kernel, tables + [field] + faces_x(), (lame, nodes, *old, *x_halos, *halos), smem=1
            )
        else:
            new_outer, *x_faces = call(
                functools.partial(outer_kernel, last), [field] + faces_x(0, last), (w, d, *old, *x_halos, *halos)
            )
        x_halos = send_x(*x_faces)
        if k == 0:
            inner, *faces = call(pack_inner_kernel, [field] + faces_y_z(8), (flat, nodes, outer))
        else:
            outer = new_outer
            inner, *faces = call(
                functools.partial(inner_kernel, last), [field] + faces_y_z(0, last), (w, d, *old, *halos, outer)
            )
        old = in_vmem(outer, inner)
        if not last:
            halos = send_y_z(*faces)
        else:
            y_hi, ends = faces
            halos = in_vmem(ring(y_hi, "gy", 1), ring(ends, "gz", 1))
        if last:
            inside = call(inside_kernel, vmem(VECS, 2 * VECS), (w, d, *old), scratch=[vmem(2 * VECS, NX * NY * NZ)])
        elif k > 0:
            grams.append(call(gram_kernel, small, old))
    sums = call(across_kernel, vmem(VECS, 4 * VECS), (w, *grams, inside, *old, ends, *x_halos, *halos))
    mixing, coarse = call(
        functools.partial(factor_kernel, n_rows),
        [small, jax.ShapeDtypeStruct((VECS, VECS), F32)],
        (all_sum(sums),),
        scratch=[vmem(ITERS + 1, VECS, VECS), vmem(VECS, VECS)],
    )
    rows_of_one = VECS * NX * NY
    basis = pl.pallas_call(
        basis_kernel,
        grid=(COMPS,),
        out_shape=jax.ShapeDtypeStruct((COMPS * rows_of_one, NZ), F32),
        in_specs=[VMEM] * 3,
        out_specs=pl.BlockSpec((rows_of_one, NZ), lambda c: (c, 0)),
        compiler_params=pltpu.CompilerParams(vmem_limit_bytes=LIMIT),
    )(mixing, *old)
    return basis.reshape(start.shape), coarse


def solution(mesh):
    in_specs = (P("gx", "gy", "gz"), P(), P(None, None, "gx", "gy", "gz"))
    out_specs = (P(None, None, "gx", "gy", "gz"), P())
    return jax.shard_map(on_device, mesh=mesh, in_specs=in_specs, out_specs=out_specs, check_vma=False)
```

```python
import functools

import jax
import jax.numpy as jnp
from jax import lax
from jax.experimental import pallas as pl
from jax.experimental.pallas import tpu as pltpu
from jax.sharding import PartitionSpec as P


ITERS = 3
BRICK = 4

COMPS, VECS, NX, NY, NZ = 3, 32, 4, 8, 128
HALF = (COMPS, VECS, NX * NY * NZ // 2)
OUTER, INNER = (0, NX - 1), (1, NX - 2)
F32 = jnp.float32

XI, XLD, XLO, XHD, XHO = 0, 2, 4, 6, 8
YM, YLD, YLO, YHD, YHO = 10, 11, 12, 13, 14
ZLD, ZLO, ZRD, ZRO = 15, 17, 19, 21
KIND = 23
LIMIT = 24 * 1024 * 1024
YCASE = (0, 1, 1, 2, 3, 4, 4, 5)
XCASE = (0, 1, 1, 2)

VMEM = pl.BlockSpec(memory_space=pltpu.VMEM)
SMEM = pl.BlockSpec(memory_space=pltpu.SMEM)


def in_vmem(*arrays):
    return [pltpu.with_memory_space_constraint(a, pltpu.VMEM) for a in arrays]


def lanes():
    return lax.broadcasted_iota(jnp.int32, (VECS, NZ), 1)


def rows(block):
    return pl.ds(pl.multiple_of(block * VECS, VECS), VECS)


def dot_t(a, b):
    return lax.dot_general(
        a, b, (((1,), (1,)), ((), ())), precision=lax.Precision.HIGHEST, preferred_element_type=F32
    )


def dot(a, b):
    return jnp.dot(a, b, precision=lax.Precision.HIGHEST, preferred_element_type=F32)


def block_of(outer, inner, c, xi, yi):
    ref = outer if xi in OUTER else inner
    start = ((xi > 1) * NY + yi) * NZ
    return ref.at[c, :, pl.ds(start, NZ)]


def emit_x(c, xi, yi, value, faces, last):
    x_lo, x_hi = faces
    half = NY // 2
    if not last:
        (x_lo if xi == 0 else x_hi)[rows(c * NY + yi), :] = value
    elif xi == 0 and yi >= half:
        x_lo[rows(c * half + yi - half), :] = value
    elif xi > 0 and yi < half:
        x_hi[rows(c * half + yi), :] = value


def emit_y_z(outer, inner, faces, last):
    lane = lanes()

    def comp(c, carry):
        ends = jnp.zeros((VECS, NZ), F32)
        for xi in range(NX):
            for yi in range(NY):
                value = block_of(outer, inner, c, xi, yi)[...]
                if yi == 0 and not last:
                    faces[1][rows(c * NX + xi), :] = value
                if yi == NY - 1:
                    faces[0][rows(c * NX + xi), :] = value
                b = xi * NY + yi
                if b:
                    value = pltpu.roll(value, 2 * b, 1)
                ends = jnp.where((lane == 2 * b) | (lane == (2 * b - 1) % NZ), value, ends)
        faces[-1][rows(c), :] = ends
        return carry

    lax.fori_loop(0, COMPS, comp, 0)


def node_phases(phase_ref):
    spread = (
        lax.broadcasted_iota(jnp.int32, (NZ // BRICK, NZ), 1) // BRICK
        == lax.broadcasted_iota(jnp.int32, (NZ // BRICK, NZ), 0)
    ).astype(F32)
    bricks = jnp.concatenate([phase_ref[0].astype(F32), jnp.zeros((6, NZ // BRICK), F32)], axis=0)
    return jnp.dot(bricks, spread, preferred_element_type=F32)


def native(xi, yi):
    return pl.ds(xi * NY + yi, VECS, stride=NX * NY)


def pack_outer_kernel(x_ref, phase_ref, nodes_ref, outer, x_lo, x_hi):
    for c in range(COMPS):
        for xi in OUTER:
            for yi in range(NY):
                value = x_ref[pl.ds(c * NX * NY * VECS + xi * NY + yi, VECS, stride=NX * NY), :]
                block_of(outer, None, c, xi, yi)[...] = value
                emit_x(c, xi, yi, value, (x_lo, x_hi), False)
    nodes = node_phases(phase_ref)
    nodes_ref[...] = nodes
    for face in (x_lo, x_hi):
        face[COMPS * NY * VECS : COMPS * NY * VECS + 8, :] = nodes


def pack_inner_kernel(x_ref, nodes_ref, outer, inner, y_hi, y_lo, ends):
    for c in range(COMPS):
        for xi in INNER:
            for yi in range(NY):
                value = x_ref[pl.ds(c * NX * NY * VECS + xi * NY + yi, VECS, stride=NX * NY), :]
                block_of(outer, inner, c, xi, yi)[...] = value
    emit_y_z(outer, inner, (y_hi, y_lo, ends), False)
    for face, blocks in ((y_hi, COMPS * NX), (y_lo, COMPS * NX), (ends, COMPS)):
        face[blocks * VECS : blocks * VECS + 8, :] = nodes_ref[...]


def weight_tables(lame_ref, own_ref, halos, w_ref, d_ref):
    hxm, hxp, hym, hyp, hzm, hzp = halos
    lane = lax.broadcasted_iota(jnp.int32, (1, NZ), 1)
    first = [lax.axis_index(a) == 0 for a in ("gx", "gy", "gz")]
    last = [lax.axis_index(a) == lax.axis_size(a) - 1 for a in ("gx", "gy", "gz")]

    def phases(ref, blocks, outside):
        found = ref[blocks * VECS : blocks * VECS + 8, :]
        found = jnp.where(outside, 0.0, found)
        return [found[j : j + 1] for j in range(2)]

    own = own_ref[...]
    own = [own[j : j + 1] for j in range(2)]
    x_m = phases(hxm, COMPS * NY, first[0])
    x_p = phases(hxp, COMPS * NY, last[0])
    y_m = phases(hym, COMPS * NX, first[1])
    y_p = phases(hyp, COMPS * NX, last[1])
    z_m = phases(hzm, COMPS, first[2])
    z_p = phases(hzp, COMPS, last[2])
    left = [jnp.where(lane == 0, pltpu.roll(z_m[j], 1, 1), pltpu.roll(own[j], 1, 1)) for j in range(2)]
    right = [
        jnp.where(lane == NZ - 1, pltpu.roll(z_p[j], NZ - 1, 1), pltpu.roll(own[j], NZ - 1, 1)) for j in range(2)
    ]
    in_l = jnp.where((lane == 0) & first[2], 0.0, 1.0)
    in_r = jnp.where((lane == NZ - 1) & last[2], 0.0, 1.0)
    in_x = [jnp.where(e[0], 0.0, 1.0) for e in (first, last)]
    in_y = [jnp.where(e[1], 0.0, 1.0) for e in (first, last)]
    tables = []
    for kind in range(2):
        pair = [lame_ref[p, 0] + (lame_ref[p, 0] + lame_ref[p, 1]) if kind else lame_ref[p, 0] for p in range(2)]

        def f(ph):
            return jnp.where(ph > 0.5, pair[1], pair[0])

        table = {}
        for j in range(2):
            here = f(own[j])
            table[XI + j] = here
            table[XLD + j] = 0.5 * (here + f(x_m[j]))
            table[XLO + j] = table[XLD + j] * in_x[0]
            table[XHD + j] = 0.5 * (here + f(x_p[j]))
            table[XHO + j] = table[XHD + j] * in_x[1]
            table[ZLD + j] = 0.5 * (here + f(left[j]))
            table[ZLO + j] = table[ZLD + j] * in_l
            table[ZRD + j] = 0.5 * (here + f(right[j]))
            table[ZRO + j] = table[ZRD + j] * in_r
        table[YM] = 0.5 * (f(own[0]) + f(own[1]))
        table[YLD] = 0.5 * (f(own[0]) + f(y_m[1]))
        table[YLO] = table[YLD] * in_y[0]
        table[YHD] = 0.5 * (f(own[1]) + f(y_p[0]))
        table[YHO] = table[YHD] * in_y[1]
        for row, value in table.items():
            w_ref[kind * KIND + row] = jnp.broadcast_to(value, (8, NZ))
        tables.append(table)
    for c in range(COMPS):
        tx, ty, tz = (tables[1 if c == d else 0] for d in range(3))
        for xc in range(3):
            for yc in range(6):
                j = yc // 3
                along_x = (tx[XLD + j] + tx[XI + j], tx[XI + j] + tx[XI + j], tx[XI + j] + tx[XHD + j])[xc]
                inner = ty[XI + j]
                along_y = (ty[YLD] + inner, inner + inner, inner + ty[YM], ty[YM] + inner, inner + inner, inner + ty[YHD])[yc]
                total = along_x + along_y + (tz[ZLD + j] + tz[ZRD + j])
                d_ref[(c * 3 + xc) * 6 + yc] = jnp.broadcast_to(total, (8, NZ))


def times(weight, value):
    return (weight[None] * value.reshape(4, 8, NZ)).reshape(VECS, NZ)


def kinds(c):
    return [jnp.where(c == d, KIND, 0) for d in range(3)]


def apply_operator(c, outer, inner, halos, w_ref, d_ref, layers, done):
    lane = lanes()
    kx, ky, kz = kinds(c)
    if halos:
        hxm, hxp, hym, hyp, hzm, hzp = halos
        ends = jnp.where(lane % 2 == 0, hzp[rows(c), :], pltpu.roll(hzm[rows(c), :], 2, 1))

    def at(xi, yi):
        return block_of(outer, inner, c, xi, yi)[...]

    for xi in layers:
        for yi in range(NY):
            j = yi // BRICK
            block = xi * NY + yi
            u = at(xi, yi)
            total = times(d_ref[(c * 3 + XCASE[xi]) * 6 + YCASE[yi]], u)
            if xi > 0:
                total -= times(w_ref[kx + XI + j], at(xi - 1, yi))
            elif halos:
                total -= times(w_ref[kx + XLO + j], hxm[rows(c * NY + yi), :])
            if xi < NX - 1:
                total -= times(w_ref[kx + XI + j], at(xi + 1, yi))
            elif halos:
                total -= times(w_ref[kx + XHO + j], hxp[rows(c * NY + yi), :])
            if yi > 0:
                total -= times(w_ref[ky + (YM if yi == BRICK else XI + j)], at(xi, yi - 1))
            elif halos:
                total -= times(w_ref[ky + YLO], hym[rows(c * NX + xi), :])
            if yi < NY - 1:
                total -= times(w_ref[ky + (YM if yi == BRICK - 1 else XI + j)], at(xi, yi + 1))
            elif halos:
                total -= times(w_ref[ky + YHO], hyp[rows(c * NX + xi), :])
            left, right = pltpu.roll(u, 1, 1), pltpu.roll(u, NZ - 1, 1)
            if halos:
                far = pltpu.roll(ends, NZ - 1 - 2 * block, 1)
                left, right = jnp.where(lane == 0, far, left), jnp.where(lane == NZ - 1, far, right)
            else:
                left, right = jnp.where(lane == 0, 0.0, left), jnp.where(lane == NZ - 1, 0.0, right)
            total -= times(w_ref[kz + ZLO + j], left)
            total -= times(w_ref[kz + ZRO + j], right)
            done(xi, yi, total)


def outer_step(w_ref, d_ref, refs, last):
    outer, inner, hxm, hxp, hym, hyp, hzm, hzp, new_outer, x_lo, x_hi = refs

    def comp(c, carry):
        def done(xi, yi, value):
            block_of(new_outer, None, c, xi, yi)[...] = value
            emit_x(c, xi, yi, value, (x_lo, x_hi), last)

        apply_operator(c, outer, inner, (hxm, hxp, hym, hyp, hzm, hzp), w_ref, d_ref, OUTER, done)
        return carry

    lax.fori_loop(0, COMPS, comp, 0)


def first_outer_kernel(lame_ref, nodes_ref, *refs):
    w_ref, d_ref = refs[8:10]
    weight_tables(lame_ref, nodes_ref, refs[2:8], w_ref, d_ref)
    outer_step(w_ref, d_ref, refs[:8] + refs[10:], False)


def outer_kernel(last, w_ref, d_ref, *refs):
    outer_step(w_ref, d_ref, refs, last)


def inner_kernel(last, w_ref, d_ref, outer, inner, hym, hyp, hzm, hzp, new_outer, new_inner, *faces):
    def comp(c, carry):
        def done(xi, yi, value):
            block_of(None, new_inner, c, xi, yi)[...] = value

        apply_operator(c, outer, inner, (None, None, hym, hyp, hzm, hzp), w_ref, d_ref, INNER, done)
        return carry

    lax.fori_loop(0, COMPS, comp, 0)
    emit_y_z(new_outer, new_inner, faces, last)


def gram_kernel(outer, inner, g_ref):
    total = jnp.zeros((VECS, VECS), F32)
    for ref in (outer, inner):
        for c in range(COMPS):
            total += dot_t(ref[c], ref[c])
    g_ref[...] = total


def inside_kernel(w_ref, d_ref, outer, inner, out_ref, pair_ref):
    def comp(c, total):
        def done(xi, yi, value):
            start = (xi * NY + yi) * NZ
            pair_ref[VECS:, start : start + NZ] = value

        apply_operator(c, outer, inner, None, w_ref, d_ref, range(NX), done)
        for xi in range(NX):
            ref, start = (outer if xi in OUTER else inner), (xi > 1) * NY * NZ
            pair_ref[:VECS, xi * NY * NZ : (xi + 1) * NY * NZ] = ref[c, :, start : start + NY * NZ]
        return total + dot_t(pair_ref[:VECS, :], pair_ref[...])

    out_ref[...] = lax.fori_loop(0, COMPS, comp, jnp.zeros((VECS, 2 * VECS), F32))


def across_kernel(w_ref, g1, g2, inside, outer, inner, own_ends, hxm, hxp, hym, hzm, out_ref):
    lane = lanes()
    half = NY // 2

    def comp(c, total):
        kx, ky, kz = kinds(c)
        mine, other = [], []
        for yi in range(NY):
            j = yi // BRICK
            xi = 0 if yi < half else NX - 1
            mine.append(block_of(outer, inner, c, xi, yi)[...])
            halo = hxm if yi < half else hxp
            other.append(times(w_ref[kx + (XLO if yi < half else XHO) + j], halo[rows(c * half + yi % half), :]))
        for xi in range(NX):
            mine.append(block_of(outer, inner, c, xi, 0)[...])
            other.append(times(w_ref[ky + YLO], hym[rows(c * NX + xi), :]))
        weight = [jnp.broadcast_to(w_ref[kz + ZLO + j][:, :1], (8, NZ)) for j in range(2)]
        which = lax.broadcasted_iota(jnp.int32, (8, NZ), 1)
        weight = jnp.where(which // 2 % NY < BRICK, weight[0], weight[1])
        weight = jnp.where((which % 2 == 0) & (which < 2 * NX * NY), weight, 0.0)
        mine.append(own_ends[rows(c), :])
        other.append(times(weight, pltpu.roll(hzm[rows(c), :], 1, 1)))
        return total + dot_t(jnp.concatenate(mine, axis=1), jnp.concatenate(other, axis=1))

    cross = lax.fori_loop(0, COMPS, comp, jnp.zeros((VECS, VECS), F32))
    both = inside[...]
    out_ref[...] = jnp.concatenate([g1[...], g2[...], both[:, :VECS], both[:, VECS:] - 2.0 * cross], axis=1)


def inverse_factor(gram):
    row = lax.broadcasted_iota(jnp.int32, (8, NZ), 0)
    col = lax.broadcasted_iota(jnp.int32, (8, NZ), 1)
    groups = VECS // 8
    cols = []
    for k in range(VECS):
        whole = jnp.broadcast_to(gram[:, k : k + 1], (VECS, NZ))
        cols.append([whole[8 * g : 8 * g + 8] for g in range(groups)])
    unit = [jnp.where(row + 8 * g == col, 1.0, 0.0).astype(F32) for g in range(groups)]

    def spread(group, r):
        return jnp.broadcast_to(group[r : r + 1], (8, NZ))

    for k in range(VECS):
        own, r = divmod(k, 8)
        scale = lax.rsqrt(spread(cols[k][own], r))
        factor = [None] * own + [cols[k][g] * scale for g in range(own, groups)]
        pivot = spread(unit[own], r) * scale
        for j in range(k + 1, VECS):
            at_j = spread(factor[j // 8], j % 8)
            for g in range(j // 8, groups):
                cols[j][g] = cols[j][g] - factor[g] * at_j
        unit[own] = jnp.where(row == r, pivot, jnp.where(row > r, unit[own] - factor[own] * pivot, unit[own]))
        for g in range(own + 1, groups):
            unit[g] = unit[g] - factor[g] * pivot
    return jnp.concatenate(unit, axis=0)[:, :VECS]


def factor_kernel(n_rows, sums_ref, mixing_ref, coarse_ref, grams_ref, turned_ref):
    for k in range(ITERS):
        grams_ref[k] = sums_ref[:, k * VECS : (k + 1) * VECS] / n_rows
    cross = sums_ref[:, ITERS * VECS :] / n_rows
    turned_ref[...] = cross.T
    grams_ref[ITERS] = 0.5 * (cross + turned_ref[...])

    def congruent(k, mixing):
        turned_ref[...] = mixing.T
        return dot(dot(mixing, grams_ref[k]), turned_ref[...])

    mixing = inverse_factor(grams_ref[0])
    for k in range(1, ITERS):
        mixing = dot(inverse_factor(congruent(k, mixing)), mixing)
    coarse_ref[...] = congruent(ITERS, mixing)
    mixing_ref[...] = mixing


def basis_kernel(mixing_ref, outer, inner, basis_ref):
    c = pl.program_id(0)
    for half, layers in ((outer, OUTER), (inner, INNER)):
        value = dot(mixing_ref[...], half[c])
        for slot, xi in enumerate(layers):
            for yi in range(NY):
                start = (slot * NY + yi) * NZ
                basis_ref[native(xi, yi), :] = value[:, start : start + NZ]


def vmem(*shape):
    return pltpu.VMEM(shape, F32)


def faces_x(extra=0, last=False):
    return [vmem(COMPS * NY * VECS // (2 if last else 1) + extra, NZ)] * 2


def faces_y_z(extra=0, last=False):
    return [vmem(COMPS * NX * VECS + extra, NZ)] * (1 if last else 2) + [vmem(COMPS * VECS + extra, NZ)]


def ring(value, axis, by):
    n = lax.axis_size(axis)
    return lax.ppermute(value, axis, [(i, (i + by) % n) for i in range(n)])


def send_x(x_lo, x_hi):
    return in_vmem(ring(x_hi, "gx", 1), ring(x_lo, "gx", -1))


def send_y_z(y_hi, y_lo, ends):
    return in_vmem(ring(y_hi, "gy", 1), ring(y_lo, "gy", -1), ring(ends, "gz", 1), ring(ends, "gz", -1))


def all_sum(value):
    value = value + lax.ppermute(value, "gy", [(i, i ^ 1) for i in range(4)])

    def along_x(by):
        pairs = []
        for i in range(32):
            x_low, core, x_high, z = i // 16, i // 8 % 2, i // 4 % 2, i % 4
            x = (2 * x_high + x_low + by) % 4
            pairs.append((i, (x % 2) * 16 + core * 8 + (x // 2) * 4 + z))
        return pairs

    def along_z(by):
        return [(i, i // 4 * 4 + (i % 4 + by) % 4) for i in range(8)]

    def along_y(by):
        return [(i, (i + by) % 4) for i in range(4)]

    for axis, pairs in ((("gy", "gz"), along_x), ("gx", along_y), ("gz", along_z)):
        parts = []
        for by in (1, 2, 3):
            parts.append(lax.ppermute(value, axis, pairs(by)))
        one, two, three = parts
        value = (value + two) + (one + three)
    return value


def call(kernel, outs, args, flops=4_000_000, scratch=(), smem=0):
    return pl.pallas_call(
        kernel,
        out_shape=outs,
        in_specs=[SMEM] * smem + [VMEM] * (len(args) - smem),
        out_specs=jax.tree.map(lambda _: VMEM, outs),
        scratch_shapes=scratch,
        cost_estimate=pl.CostEstimate(flops=flops, bytes_accessed=3_000_000, transcendentals=0),
        compiler_params=pltpu.CompilerParams(vmem_limit_bytes=LIMIT),
    )(*args)


def on_device(phase, lame, start):
    n_rows = 3.0 * start.shape[2] * start.shape[3] * start.shape[4]
    for axis in ("gx", "gy", "gz"):
        n_rows *= lax.axis_size(axis)
    field, small = vmem(*HALF), vmem(VECS, VECS)
    (flat,) = in_vmem(start.reshape(-1, NZ))
    grams = []
    for k in range(ITERS + 1):
        last = k == ITERS
        if k == 0:
            nodes, outer, *x_faces = call(pack_outer_kernel, [vmem(8, NZ), field] + faces_x(8), (flat, phase))
        elif k == 1:
            tables = [vmem(2 * KIND, 8, NZ), vmem(54, 8, NZ)]
            w, d, new_outer, *x_faces = call(
                first_outer_kernel, tables + [field] + faces_x(), (lame, nodes, *old, *x_halos, *halos), smem=1
            )
        else:
            new_outer, *x_faces = call(
                functools.partial(outer_kernel, last), [field] + faces_x(0, last), (w, d, *old, *x_halos, *halos)
            )
        x_halos = send_x(*x_faces)
        if k == 0:
            inner, *faces = call(pack_inner_kernel, [field] + faces_y_z(8), (flat, nodes, outer))
        else:
            outer = new_outer
            inner, *faces = call(
                functools.partial(inner_kernel, last), [field] + faces_y_z(0, last), (w, d, *old, *halos, outer)
            )
        old = in_vmem(outer, inner)
        if not last:
            halos = send_y_z(*faces)
        else:
            y_hi, ends = faces
            halos = in_vmem(ring(y_hi, "gy", 1), ring(ends, "gz", 1))
        if last:
            inside = call(inside_kernel, vmem(VECS, 2 * VECS), (w, d, *old), scratch=[vmem(2 * VECS, NX * NY * NZ)])
        elif k > 0:
            grams.append(call(gram_kernel, small, old))
    sums = call(across_kernel, vmem(VECS, 4 * VECS), (w, *grams, inside, *old, ends, *x_halos, *halos))
    mixing, coarse = call(
        functools.partial(factor_kernel, n_rows),
        [small, jax.ShapeDtypeStruct((VECS, VECS), F32)],
        (all_sum(sums),),
        scratch=[vmem(ITERS + 1, VECS, VECS), vmem(VECS, VECS)],
    )
    rows_of_one = VECS * NX * NY
    basis = pl.pallas_call(
        basis_kernel,
        grid=(COMPS,),
        out_shape=jax.ShapeDtypeStruct((COMPS * rows_of_one, NZ), F32),
        in_specs=[VMEM] * 3,
        out_specs=pl.BlockSpec((rows_of_one, NZ), lambda c: (c, 0)),
        compiler_params=pltpu.CompilerParams(vmem_limit_bytes=LIMIT),
    )(mixing, *old)
    return basis.reshape(start.shape), coarse


def solution(mesh):
    in_specs = (P("gx", "gy", "gz"), P(), P(None, None, "gx", "gy", "gz"))
    out_specs = (P(None, None, "gx", "gy", "gz"), P())
    return jax.shard_map(on_device, mesh=mesh, in_specs=in_specs, out_specs=out_specs, check_vma=False)
```
